32 devices in a mesh: dp: 1 (over z), tp: 4 (over y), fsdp: 8 (over x, core).
Axes of the slice: x: 4, y: 4, z: 1, core: 2. Of those that a mesh axis runs over, the one named last changes fastest.
The devices are a block of a 4x4x8 slice.
Arguments:
- hidden: bfloat16 [64, 512, 2048], P(('dp', 'fsdp'))
- seq_lens: int32 [64], P(('dp', 'fsdp'))
- w_qkv: bfloat16 [2, 2048, 3, 32, 64], P(None, 'fsdp', None, 'tp')
- b_qkv: bfloat16 [2, 3, 2048], P(None, None, ('tp', 'fsdp'))
- w_proj: bfloat16 [2, 2048, 2048], P(None, ('tp', 'fsdp'))
- w_up: bfloat16 [2, 2048, 8192], P(None, 'fsdp', 'tp')
- b_up: bfloat16 [2, 8192], P(None, ('tp', 'fsdp'))
- w_down: bfloat16 [2, 8192, 2048], P(None, ('tp', 'fsdp'))
- b_resid: bfloat16 [2, 2, 2048], P(None, None, 'fsdp')
- ln_params: float32 [2, 4, 2048], P(None, None, 'fsdp')
Outputs:
- output: bfloat16 [64, 512, 2048], P(('dp', 'fsdp'))
All inputs are finite; a program needn't handle non-finite values.
Results may differ from the reference program's by a relative error of at most 0.0175426.
Values are sent between devices in bfloat16 or wider.
A program may use at most 768 MiB of HBM per device.

```python
import jax
import jax.numpy as jnp
from jax import lax

D_MODEL = 2048
N_HEADS = 32
SEQ_LEN = 512
BATCH_ROWS = 64
LAYERS = 2
HEAD_DIM = D_MODEL // N_HEADS
FF_DIM = 4 * D_MODEL


def setup_inputs(seed: int = 0, part: int = 0) -> dict:
    root_key = jax.random.key(seed)
    sub_keys = jax.random.split(root_key, 9)
    part_key = jax.random.fold_in(sub_keys[8], part)
    hid_key, len_key = jax.random.split(part_key)
    hidden = jax.random.normal(hid_key, (BATCH_ROWS, SEQ_LEN, D_MODEL), jnp.float32).astype(jnp.bfloat16)
    drawn_lens = jax.random.randint(len_key, (BATCH_ROWS,), SEQ_LEN // 4, SEQ_LEN + 1, jnp.int32)
    seq_lens = jnp.concatenate([jnp.array([SEQ_LEN, SEQ_LEN // 4], jnp.int32), drawn_lens[2:]])

    def normal_w(rng_key, shape, w_scale):
        return (jax.random.normal(rng_key, shape, jnp.float32) * w_scale).astype(jnp.bfloat16)

    qkv_scale = jnp.array([1.5, 1.5, 1.0], jnp.float32)[:, None, None]
    w_qkv = normal_w(sub_keys[0], (LAYERS, D_MODEL, 3, N_HEADS, HEAD_DIM), D_MODEL ** -0.5 * qkv_scale)
    b_qkv = normal_w(sub_keys[1], (LAYERS, 3, D_MODEL), 0.5)
    w_proj = normal_w(sub_keys[2], (LAYERS, D_MODEL, D_MODEL), D_MODEL ** -0.5)
    w_up = normal_w(sub_keys[3], (LAYERS, D_MODEL, FF_DIM), D_MODEL ** -0.5)
    b_up = normal_w(sub_keys[4], (LAYERS, FF_DIM), 0.5)
    w_down = normal_w(sub_keys[5], (LAYERS, FF_DIM, D_MODEL), FF_DIM ** -0.5)
    b_resid = normal_w(sub_keys[6], (LAYERS, 2, D_MODEL), 0.3)
    ln_base = jnp.array([1.0, 0.0, 1.0, 0.0], jnp.float32)[None, :, None]
    ln_params = ln_base + 0.3 * jax.random.normal(sub_keys[7], (LAYERS, 4, D_MODEL), jnp.float32)
    return dict(hidden=hidden, seq_lens=seq_lens, w_qkv=w_qkv, b_qkv=b_qkv, w_proj=w_proj, w_up=w_up, b_up=b_up, w_down=w_down, b_resid=b_resid, ln_params=ln_params)


def layer_norm(acts_in, ln_gain, ln_shift):
    as_f32 = acts_in.astype(jnp.float32)
    row_mean = jnp.mean(as_f32, axis=-1, keepdims=True)
    centered = as_f32 - row_mean
    row_var = jnp.mean(centered * centered, axis=-1, keepdims=True)
    return (centered * lax.rsqrt(row_var + 1e-5) * ln_gain + ln_shift).astype(jnp.bfloat16)


def one_layer(seq_row, length, layer_params):
    w_qkv, b_qkv, w_proj, w_up, b_up, w_down, b_resid, ln_params = layer_params
    normed = layer_norm(seq_row, ln_params[0], ln_params[1])
    qkv_out = jnp.dot(normed, w_qkv.reshape(D_MODEL, 3 * D_MODEL), preferred_element_type=jnp.float32)
    qkv_out = (qkv_out + b_qkv.reshape(3 * D_MODEL).astype(jnp.float32)).astype(jnp.bfloat16)
    qkv_out = qkv_out.reshape(SEQ_LEN, 3, N_HEADS, HEAD_DIM).astype(jnp.float32)
    scores = jnp.einsum('qhe,khe->hqk', qkv_out[:, 0], qkv_out[:, 1]) * HEAD_DIM ** -0.5
    positions = jnp.arange(SEQ_LEN)
    allowed = (positions[None, :] <= positions[:, None]) & (positions[None, :] < length)
    scores = jnp.where(allowed[None], scores, -1e30)
    attn_probs = jax.nn.softmax(scores, axis=-1).astype(jnp.bfloat16).astype(jnp.float32)
    context = jnp.einsum('hqk,khe->qhe', attn_probs, qkv_out[:, 2]).astype(jnp.bfloat16)
    attn_out = jnp.dot(context.reshape(SEQ_LEN, D_MODEL), w_proj, preferred_element_type=jnp.float32)
    mid_state = (seq_row.astype(jnp.float32) + attn_out + b_resid[0].astype(jnp.float32)).astype(jnp.bfloat16)
    normed_mid = layer_norm(mid_state, ln_params[2], ln_params[3])
    up_out = jnp.dot(normed_mid, w_up, preferred_element_type=jnp.float32) + b_up.astype(jnp.float32)
    hidden_up = jnp.maximum(up_out, 0.0).astype(jnp.bfloat16)
    down_out = jnp.dot(hidden_up, w_down, preferred_element_type=jnp.float32)
    return (mid_state.astype(jnp.float32) + down_out + b_resid[1].astype(jnp.float32)).astype(jnp.bfloat16)


def reference(hidden, seq_lens, w_qkv, b_qkv, w_proj, w_up, b_up, w_down, b_resid, ln_params):
    stacked = (w_qkv, b_qkv, w_proj, w_up, b_up, w_down, b_resid, ln_params)

    def one_row(row_item):
        seq_row, length = row_item

        def layer_step(state_row, layer_params):
            return one_layer(state_row, length, layer_params), None

        return lax.scan(layer_step, seq_row, stacked)[0]

    return lax.map(one_row, (hidden, seq_lens))
```

```python
import functools

import jax
import jax.numpy as jnp
from jax import lax
from jax.experimental import pallas as pl
from jax.experimental.pallas import tpu as pltpu
from jax.sharding import PartitionSpec as P


BOTH = ('tp', 'fsdp')
TILE = 512


def layer_norm(acts_in, ln_gain, ln_shift):
    as_f32 = acts_in.astype(jnp.float32)
    row_mean = jnp.mean(as_f32, axis=-1, keepdims=True)
    centered = as_f32 - row_mean
    row_var = jnp.mean(centered * centered, axis=-1, keepdims=True)
    return (centered * lax.rsqrt(row_var + 1e-5) * ln_gain + ln_shift).astype(jnp.bfloat16)


def attn_kernel(head_dim, heads, lens_ref, q_ref, k_ref, v_ref, o_ref):
    seq_len = q_ref.shape[1]
    half = seq_len // 2
    length = lens_ref[pl.program_id(0)]
    last = jnp.minimum(lax.broadcasted_iota(jnp.int32, (1, seq_len), 1), length - 1)
    key = lax.broadcasted_iota(jnp.int32, (half, seq_len), 0)
    early_ok = key <= last
    late_ok = key[:, :half] + half <= last[:, half:]
    keys_by_queries = (((1,), (1,)), ((), ()))
    over_keys = (((0,), (0,)), ((), ()))
    columns = [slice(h * head_dim, (h + 1) * head_dim) for h in range(heads)]
    scores = []
    for c in columns:
        q = q_ref[0, :, c] * jnp.bfloat16(head_dim ** -0.5)
        early = lax.dot_general(k_ref[0, :half, c], q, keys_by_queries, preferred_element_type=jnp.float32)
        late = lax.dot_general(k_ref[0, half:, c], q[half:], keys_by_queries, preferred_element_type=jnp.float32)
        scores.append((early, late))
    outs = []
    for c, (early, late) in zip(columns, scores):
        early = jnp.where(early_ok, early, -1e30)
        late = jnp.where(late_ok, late, -1e30)
        top = jnp.max(early, axis=0, keepdims=True)
        late_top = jnp.maximum(top[:, half:], jnp.max(late, axis=0, keepdims=True))
        early = jnp.exp(early - jnp.concatenate([top[:, :half], late_top], axis=1))
        late = jnp.exp(late - late_top)
        total = jnp.sum(early, axis=0, keepdims=True)
        late_total = total[:, half:] + jnp.sum(late, axis=0, keepdims=True)
        scale = 1.0 / jnp.concatenate([total[:, :half], late_total], axis=1)
        early = (early * scale).astype(jnp.bfloat16)
        late = (late * scale[:, half:]).astype(jnp.bfloat16)
        v = v_ref[0, :, c]
        first = lax.dot_general(v[:half], early[:, :half], over_keys, preferred_element_type=jnp.float32)
        second = lax.dot_general(v, jnp.concatenate([early[:, half:], late], axis=0), over_keys, preferred_element_type=jnp.float32)
        outs.append(jnp.concatenate([first, second], axis=1))
    o_ref[0] = jnp.concatenate(outs, axis=0).T.astype(jnp.bfloat16)


def attend(qkv, lens, share, head_dim):
    seqs, seq_len, total = qkv.shape
    width = total // 3
    block = 256
    per = share // block
    spec = lambda part: pl.BlockSpec((1, seq_len, block), lambda s, g, h, lens: (s, 0, (g * 3 + part) * per + h))
    return pl.pallas_call(
        functools.partial(attn_kernel, head_dim, block // head_dim),
        out_shape=jax.ShapeDtypeStruct((seqs, seq_len, width), jnp.bfloat16),
        grid_spec=pltpu.PrefetchScalarGridSpec(
            num_scalar_prefetch=1,
            grid=(seqs, width // share, per),
            in_specs=[spec(0), spec(1), spec(2)],
            out_specs=pl.BlockSpec((1, seq_len, block), lambda s, g, h, lens: (s, 0, g * per + h)),
        ),
        compiler_params=pltpu.CompilerParams(vmem_limit_bytes=40 * 1024 * 1024),
        cost_estimate=pl.CostEstimate(flops=16 * seqs * seq_len * seq_len * width, bytes_accessed=8 * seqs * seq_len * width, transcendentals=seqs * seq_len * seq_len * width // head_dim),
    )(lens, qkv, qkv, qkv)


def mm_kernel(relu, steps, x_ref, w_ref, b_ref, *refs):
    resid_ref = refs[0] if len(refs) == 3 else None
    o_ref, acc_ref = refs[-2:]
    k = pl.program_id(1)
    rows = x_ref.shape[0]
    w = w_ref[...].reshape(-1, w_ref.shape[2])
    half = min(512, rows)

    def start(r):
        base = jnp.broadcast_to(b_ref[...], (half, w.shape[1]))
        return base if resid_ref is None else base + resid_ref[r, :].astype(jnp.float32)

    for r0 in range(0, rows, half):
        r = pl.ds(r0, half)
        if steps == 1:
            total = jnp.dot(x_ref[r, :], w, preferred_element_type=jnp.float32) + start(r)
            o_ref[r, :] = (jnp.maximum(total, 0.0) if relu else total).astype(o_ref.dtype)
            continue

        @pl.when(k == 0)
        def _():
            acc_ref[r, :] = start(r)

        acc_ref[r, :] += jnp.dot(x_ref[r, :], w, preferred_element_type=jnp.float32)

        @pl.when(k == steps - 1)
        def _():
            o_ref[r, :] = acc_ref[r, :].astype(o_ref.dtype)


def matmul(x, w, bias, n, steps, w_block, w_index, resid=None, relu=False, first=0):
    rows, depth = x.shape
    tile = w_block[2]
    in_specs = [
        pl.BlockSpec((rows, depth // steps), lambda j, k: (0, k)),
        pl.BlockSpec(w_block, w_index),
        pl.BlockSpec((1, tile), lambda j, k: (0, first + j)),
    ]
    args = [x, w, bias.reshape(1, -1)]
    if resid is not None:
        in_specs.append(pl.BlockSpec((rows, tile), lambda j, k: (0, first + j)))
        args.append(resid)
    return pl.pallas_call(
        functools.partial(mm_kernel, relu, steps),
        out_shape=jax.ShapeDtypeStruct((rows, n), jnp.bfloat16),
        grid=(n // tile, steps),
        in_specs=in_specs,
        out_specs=pl.BlockSpec((rows, tile), lambda j, k: (0, j)),
        scratch_shapes=[pltpu.VMEM((rows, tile) if steps > 1 else (8, 128), jnp.float32)],
        compiler_params=pltpu.CompilerParams(vmem_limit_bytes=48 * 1024 * 1024),
        cost_estimate=pl.CostEstimate(flops=2 * rows * depth * n, bytes_accessed=2 * (depth * n + rows * (depth + n)), transcendentals=0),
    )(*args)


def place(out, x, step, column, size, total, width):
    rows, tile = x.shape
    piece = rows // 4

    def kernel(x_ref, *refs):
        o_ref, sem = refs[-2:]
        owner = lax.rem(lax.axis_index('tp') + step + size, size)
        row = pl.multiple_of(owner * rows + pl.program_id(0) * piece, piece)
        copy = pltpu.make_async_copy(x_ref, o_ref.at[pl.ds(row, piece), pl.ds(column * tile, tile)], sem)
        copy.start()
        copy.wait()

    whole = pl.BlockSpec(memory_space=pltpu.HBM)
    return pl.pallas_call(
        kernel,
        out_shape=jax.ShapeDtypeStruct((total, width), x.dtype),
        grid=(rows // piece,),
        in_specs=[pl.BlockSpec((piece, tile), lambda i: (i, 0))] + ([] if out is None else [whole]),
        out_specs=whole,
        scratch_shapes=[pltpu.SemaphoreType.DMA],
        input_output_aliases={} if out is None else {1: 0},
        compiler_params=pltpu.CompilerParams(vmem_limit_bytes=8 * 1024 * 1024),
        cost_estimate=pl.CostEstimate(flops=x.size, bytes_accessed=4 * x.size, transcendentals=0),
    )(*([x] if out is None else [x, out]))


def solution(mesh):
    rows_spec = P(('dp', 'fsdp'), None, None)
    in_specs = (rows_spec, P(('dp', 'fsdp')), P(None, 'fsdp', None, 'tp', None), P(None, None, ('tp', 'fsdp')), P(None, ('tp', 'fsdp'), None), P(None, 'fsdp', 'tp'), P(None, ('tp', 'fsdp')), P(None, ('tp', 'fsdp'), None), P(None, None, 'fsdp'), P(None, None, 'fsdp'))
    tp = mesh.shape['tp']
    fs = mesh.shape['fsdp']

    def per_device(hidden, seq_lens, w_qkv, b_qkv, w_proj, w_up, b_up, w_down, b_resid, ln_params):
        n_layers, rows, _, local_heads, head_dim = w_qkv.shape
        seq_len, d_model = hidden.shape[1:]
        share = local_heads * head_dim
        ff = w_up.shape[2]
        proj_rows = w_proj.shape[1]
        my_seqs = hidden.shape[0] // tp
        me = lax.axis_index('tp')

        def gather(x):
            return lax.all_gather(x, BOTH, axis=0, tiled=False)

        qkv_loc = [w_qkv[l].reshape(rows, 3 * share) for l in range(n_layers)]
        groups = rows // proj_rows
        proj_loc = [w_proj[l].reshape(proj_rows, groups, -1).transpose(1, 0, 2).reshape(rows, -1) for l in range(n_layers)]
        assert proj_loc[0].shape[1] == TILE and n_layers == 2
        g1 = gather(qkv_loc[0])
        g2 = gather(jnp.concatenate([w_up[0], w_down[0], qkv_loc[1], proj_loc[0]], axis=1))
        g3 = gather(jnp.concatenate([w_up[1], proj_loc[1]], axis=1))
        g4 = gather(w_down[1])
        wide_tiles = d_model // TILE
        ff_tiles = ff // TILE
        qkv_at = [(g1, 0), (g2, ff_tiles + wide_tiles)]
        proj_at = [(g2, ff_tiles + wide_tiles + 3 * share // TILE), (g3, ff_tiles)]
        up_at = [(g2, 0), (g3, 0)]
        down_at = [(g2, ff_tiles), (g4, 0)]

        small = gather(jnp.concatenate([b_qkv.reshape(n_layers, -1), b_up], axis=1)).astype(jnp.float32)
        small = small.reshape(tp, fs, n_layers, -1)
        piece = share // fs
        qkv_bias = small[..., :3 * piece].reshape(tp, fs, n_layers, 3, piece).transpose(2, 0, 3, 1, 4).reshape(n_layers, -1)
        up_bias = small[..., 3 * piece:].transpose(2, 0, 1, 3).reshape(n_layers, -1)
        wide = lax.all_gather(jnp.concatenate([ln_params, b_resid.astype(jnp.float32)], axis=1), 'fsdp', axis=2, tiled=True)

        current = lax.dynamic_slice_in_dim(hidden, me * my_seqs, my_seqs, 0).reshape(my_seqs * seq_len, d_model)
        lens = lax.dynamic_slice_in_dim(seq_lens, me * my_seqs, my_seqs, 0)

        per = 3 * share // TILE
        for l in range(n_layers):
            normed = layer_norm(current, wide[l, 0], wide[l, 1])
            w, c0 = qkv_at[l]
            qkv = matmul(normed, w, qkv_bias[l], tp * 3 * share, 1, (fs, rows, TILE), lambda j, k, c0=c0: (j // per, 0, c0 + j % per))
            context = attend(qkv.reshape(my_seqs, seq_len, -1), lens, share, head_dim)
            w, c0 = proj_at[l]
            mid = matmul(context.reshape(my_seqs * seq_len, -1), w, wide[l, 4], d_model, 1, (tp * fs, proj_rows, TILE), lambda j, k, c0=c0: (0, j, c0), resid=current)
            normed_mid = layer_norm(mid, wide[l, 2], wide[l, 3])
            w, c0 = up_at[l]
            u = matmul(normed_mid, w, up_bias[l], tp * ff, 1, (fs, rows, TILE), lambda j, k, c0=c0: (j // ff_tiles, 0, c0 + j % ff_tiles), relu=True)
            w, c0 = down_at[l]
            down = lambda first, n: matmul(u, w, wide[l, 5], n, tp, (fs, rows, TILE), lambda j, k: (k, 0, c0 + first + j), resid=mid, first=first)
            if l + 1 < n_layers:
                current = down(0, d_model)
        plus = [(i, (i + 1) % tp) for i in range(tp)]
        minus = [(i, (i - 1) % tp) for i in range(tp)]
        blocks = []
        for j in range(wide_tiles):
            own = down(j, TILE)
            right = lax.ppermute(own, 'tp', plus)
            left = lax.ppermute(own, 'tp', minus)
            blocks += [(0, j, own), (-1, j, right), (1, j, left)]
        for j in range(wide_tiles):
            here, perm = (blocks[3 * j + 1], plus) if j < wide_tiles // 2 else (blocks[3 * j + 2], minus)
            blocks.append((2, j, lax.ppermute(here[2], 'tp', perm)))
        out = None
        for step, j, x in blocks:
            out = place(out, x, step, j, tp, tp * my_seqs * seq_len, d_model)
        return out.reshape(hidden.shape)

    return jax.shard_map(per_device, mesh=mesh, in_specs=in_specs, out_specs=rows_spec, check_vma=False)
```

```python
import functools

import jax
import jax.numpy as jnp
from jax import lax
from jax.experimental import pallas as pl
from jax.experimental.layout import Layout, with_layout_constraint
from jax.experimental.pallas import tpu as pltpu
from jax.sharding import PartitionSpec as P


BOTH = ('tp', 'fsdp')
TILE = 512


def layer_norm(acts_in, ln_gain, ln_shift):
    as_f32 = acts_in.astype(jnp.float32)
    row_mean = jnp.mean(as_f32, axis=-1, keepdims=True)
    centered = as_f32 - row_mean
    row_var = jnp.mean(centered * centered, axis=-1, keepdims=True)
    return (centered * lax.rsqrt(row_var + 1e-5) * ln_gain + ln_shift).astype(jnp.bfloat16)


def attn_kernel(head_dim, heads, lens_ref, q_ref, k_ref, v_ref, o_ref):
    seq_len = q_ref.shape[1]
    half = seq_len // 2
    length = lens_ref[pl.program_id(0)]
    last = jnp.minimum(lax.broadcasted_iota(jnp.int32, (1, seq_len), 1), length - 1)
    key = lax.broadcasted_iota(jnp.int32, (half, seq_len), 0)
    early_ok = key <= last
    late_ok = key[:, :half] + half <= last[:, half:]
    keys_by_queries = (((1,), (1,)), ((), ()))
    over_keys = (((0,), (0,)), ((), ()))
    columns = [slice(h * head_dim, (h + 1) * head_dim) for h in range(heads)]
    scores = []
    for c in columns:
        q = q_ref[0, :, c] * jnp.bfloat16(head_dim ** -0.5)
        early = lax.dot_general(k_ref[0, :half, c], q, keys_by_queries, preferred_element_type=jnp.float32)
        late = lax.dot_general(k_ref[0, half:, c], q[half:], keys_by_queries, preferred_element_type=jnp.float32)
        scores.append((early, late))
    outs = []
    for c, (early, late) in zip(columns, scores):
        early = jnp.where(early_ok, early, -1e30)
        late = jnp.where(late_ok, late, -1e30)
        top = jnp.max(early, axis=0, keepdims=True)
        late_top = jnp.maximum(top[:, half:], jnp.max(late, axis=0, keepdims=True))
        early = jnp.exp(early - jnp.concatenate([top[:, :half], late_top], axis=1))
        late = jnp.exp(late - late_top)
        total = jnp.sum(early, axis=0, keepdims=True)
        late_total = total[:, half:] + jnp.sum(late, axis=0, keepdims=True)
        scale = 1.0 / jnp.concatenate([total[:, :half], late_total], axis=1)
        early = (early * scale).astype(jnp.bfloat16)
        late = (late * scale[:, half:]).astype(jnp.bfloat16)
        v = v_ref[0, :, c]
        first = lax.dot_general(v[:half], early[:, :half], over_keys, preferred_element_type=jnp.float32)
        second = lax.dot_general(v, jnp.concatenate([early[:, half:], late], axis=0), over_keys, preferred_element_type=jnp.float32)
        outs.append(jnp.concatenate([first, second], axis=1))
    o_ref[0] = jnp.concatenate(outs, axis=0).T.astype(jnp.bfloat16)


def attend(qkv, lens, share, head_dim):
    seqs, seq_len, total = qkv.shape
    width = total // 3
    block = 256
    per = share // block
    spec = lambda part: pl.BlockSpec((1, seq_len, block), lambda s, g, h, lens: (s, 0, (g * 3 + part) * per + h))
    return pl.pallas_call(
        functools.partial(attn_kernel, head_dim, block // head_dim),
        out_shape=jax.ShapeDtypeStruct((seqs, seq_len, width), jnp.bfloat16),
        grid_spec=pltpu.PrefetchScalarGridSpec(
            num_scalar_prefetch=1,
            grid=(seqs, width // share, per),
            in_specs=[spec(0), spec(1), spec(2)],
            out_specs=pl.BlockSpec((1, seq_len, block), lambda s, g, h, lens: (s, 0, g * per + h)),
        ),
        compiler_params=pltpu.CompilerParams(vmem_limit_bytes=60 * 1024 * 1024),
        cost_estimate=pl.CostEstimate(flops=16 * seqs * seq_len * seq_len * width, bytes_accessed=8 * seqs * seq_len * width, transcendentals=seqs * seq_len * seq_len * width // head_dim),
    )(lens, qkv, qkv, qkv)


def mm_kernel(relu, steps, has_resid, has_norm, x_ref, w_ref, b_ref, *refs):
    resid_ref = refs[0] if has_resid else None
    o_ref, acc_ref = refs[-2:]
    k = pl.program_id(1)
    if has_norm:
        ln_ref, raw_ref, x_ref = refs[0], x_ref, acc_ref
        chunk = 128

        @pl.when(pl.program_id(0) == 0)
        def _():
            def normalise(i, carry):
                r = pl.ds(pl.multiple_of(i * chunk, chunk), chunk)
                x_ref[r, :] = layer_norm(raw_ref[r, :], ln_ref[0:1, :], ln_ref[1:2, :])
                return carry

            lax.fori_loop(0, raw_ref.shape[0] // chunk, normalise, 0)

    rows = x_ref.shape[0]
    w = w_ref[...].reshape(-1, w_ref.shape[2])
    half = min(512, rows)

    def start(r):
        base = jnp.broadcast_to(b_ref[...], (half, w.shape[1]))
        return base if resid_ref is None else base + resid_ref[r, :].astype(jnp.float32)

    for r0 in range(0, rows, half):
        r = pl.ds(r0, half)
        if steps == 1:
            total = jnp.dot(x_ref[r, :], w, preferred_element_type=jnp.float32) + start(r)
            o_ref[r, :] = (jnp.maximum(total, 0.0) if relu else total).astype(o_ref.dtype)
            continue

        @pl.when(k == 0)
        def _():
            acc_ref[r, :] = start(r)

        acc_ref[r, :] += jnp.dot(x_ref[r, :], w, preferred_element_type=jnp.float32)

        @pl.when(k == steps - 1)
        def _():
            o_ref[r, :] = acc_ref[r, :].astype(o_ref.dtype)


def matmul(x, w, bias, n, steps, w_block, w_index, resid=None, relu=False, first=0, tiles=None, norm=None, vmem=60):
    rows, depth = x.shape
    tile = w_block[2]
    in_specs = [
        pl.BlockSpec((rows, depth // steps), lambda j, k: (0, k)),
        pl.BlockSpec(w_block, w_index),
        pl.BlockSpec((1, tile), lambda j, k: (0, first + j)),
    ]
    args = [x, w, bias.reshape(1, -1)]
    if resid is not None:
        in_specs.append(pl.BlockSpec((rows, tile), lambda j, k: (0, first + j)))
        args.append(resid)
    scratch = pltpu.VMEM((rows, tile) if steps > 1 else (8, 128), jnp.float32)
    if norm is not None:
        in_specs.append(pl.BlockSpec((2, depth), lambda j, k: (0, 0)))
        args.append(norm)
        scratch = pltpu.VMEM((rows, depth), jnp.bfloat16)
    tiles = tiles or n // tile
    return pl.pallas_call(
        functools.partial(mm_kernel, relu, steps, resid is not None, norm is not None),
        out_shape=jax.ShapeDtypeStruct((rows, n), jnp.bfloat16),
        grid=(tiles, steps),
        in_specs=in_specs,
        out_specs=pl.BlockSpec((rows, tile), lambda j, k: (0, j)),
        scratch_shapes=[scratch],
        compiler_params=pltpu.CompilerParams(vmem_limit_bytes=vmem * 1024 * 1024),
        cost_estimate=pl.CostEstimate(flops=2 * rows * depth * tiles * tile, bytes_accessed=2 * (depth * tiles * tile + rows * (depth + tiles * tile)), transcendentals=0),
    )(*args)


def place(out, blocks, size, total, width):
    n = len(blocks)
    rows, tile = blocks[0][2].shape

    def kernel(*refs):
        o_ref, sems = refs[-2:]
        copies = []
        for i, (step, column, _) in enumerate(blocks):
            owner = lax.rem(lax.axis_index('tp') + step + size, size)
            row = pl.multiple_of(owner * rows, rows)
            copy = pltpu.make_async_copy(refs[i], o_ref.at[pl.ds(row, rows), pl.ds(column * tile, tile)], sems.at[i])
            copy.start()
            copies.append(copy)
        for copy in copies:
            copy.wait()

    whole = pl.BlockSpec(memory_space=pltpu.HBM)
    args = [x for _, _, x in blocks] + ([] if out is None else [out])
    return pl.pallas_call(
        kernel,
        out_shape=jax.ShapeDtypeStruct((total, width), args[0].dtype),
        in_specs=[pl.BlockSpec(memory_space=pltpu.VMEM)] * n + ([] if out is None else [whole]),
        out_specs=whole,
        scratch_shapes=[pltpu.SemaphoreType.DMA((n,))],
        input_output_aliases={} if out is None else {n: 0},
        compiler_params=pltpu.CompilerParams(vmem_limit_bytes=24 * 1024 * 1024),
        cost_estimate=pl.CostEstimate(flops=n * rows * tile, bytes_accessed=4 * n * rows * tile, transcendentals=0),
    )(*args)


def gather_kernel(ny, nx, loads, n_in, *refs):
    ins = refs[:n_in]
    small_ref = refs[n_in]
    out, small_out, *packed = refs[n_in + 1:n_in + 1 + 2 + len(loads) - 1]
    rest = refs[n_in + 1 + 2 + len(loads) - 1:]
    bufs, (load_sem, store_sem, send_sem, recv_sem, small_send, small_recv) = rest[:len(loads)], rest[len(loads):]
    shard = bufs[0]
    rows = shard.shape[0]
    y = lax.axis_index('tp')
    f = lax.axis_index('fsdp')
    x = lax.div(f, 2)
    core = lax.rem(f, 2)
    at_y = lambda d: lax.rem(y + d + ny, ny)
    at_x = lambda d: lax.rem(x + d + nx, nx)
    slot = lambda dy, dx: (at_y(dy) * nx + at_x(dx)) * 2 + core
    near = lambda dim, d: {'tp': at_y(d), 'fsdp': f} if dim == 'y' else {'tp': y, 'fsdp': at_x(d) * 2 + core}
    partner = {'tp': y, 'fsdp': x * 2 + 1 - core}

    barrier = pltpu.get_barrier_semaphore()
    for dev in (near('x', 1), near('x', -1), near('y', 1), near('y', -1), partner):
        pl.semaphore_signal(barrier, inc=1, device_id=dev, device_id_type=pl.DeviceIdType.MESH)

    fills = []
    for b, pieces in enumerate(loads):
        for which, layer, c0, width, d0 in pieces:
            src = ins[which] if layer is None else ins[which].at[layer]
            fills.append((b, pltpu.make_async_copy(src.at[:, pl.ds(c0, width)], bufs[b].at[:, pl.ds(d0, width)], load_sem.at[len(fills)])))
    for _, fill in fills:
        fill.start()
    for b, fill in fills:
        if b == 0:
            fill.wait()
    stores = [pltpu.make_async_copy(shard, out.at[slot(0, 0)], store_sem.at[0]),
              pltpu.make_async_copy(small_ref, small_out.at[core, y, x], store_sem.at[1])]
    for store in stores:
        store.start()
    pl.semaphore_wait(barrier, 5)

    sends = {}
    order = []

    def send(key, dev, dp, dq, r0, n):
        colour = key[0]
        where = slot(dq, dp) if colour == 0 else slot(dp, dq)
        r = pl.ds(colour * (rows // 2) + r0, n)
        src = shard.at[r] if (dp, dq) == (0, 0) else out.at[where, r]
        i = len(order)
        copy = pltpu.make_async_remote_copy(src, out.at[where, r], send_sem.at[i], recv_sem.at[i], device_id=dev, device_id_type=pl.DeviceIdType.MESH)
        copy.start()
        sends[key] = copy
        order.append(key)

    half, quarter = rows // 2, rows // 4
    dims = ('xy', 'yx')
    got = lambda *key: sends[key].wait_recv()

    def full(c, phase, dp):
        for d in (1, -1):
            send((c, phase, dp, d, 'full'), near(dims[c][phase], d), dp, 0, 0, half)

    def onward(c, phase, dp):
        for d, r0 in ((1, 0), (-1, quarter)):
            pos = (-d, 0) if phase == 0 else (dp, -d)
            send((c, phase, dp, d, 'part'), near(dims[c][phase], d), *pos, r0, quarter)

    def wait_full(c, phase, dp):
        got(c, phase, dp, 1, 'full')
        got(c, phase, dp, -1, 'full')

    def wait_part(c, phase, dp):
        got(c, phase, dp, 1, 'part')
        got(c, phase, dp, -1, 'part')

    def across(c, dp, dq):
        send((c, 'core', dp, dq), partner, dp, dq, 0, half)

    both = (0, 1)
    smalls = []

    def small(src, dst, dev):
        i = len(smalls)
        copy = pltpu.make_async_remote_copy(src, dst, small_send.at[i], small_recv.at[i], device_id=dev, device_id_type=pl.DeviceIdType.MESH)
        copy.start()
        smalls.append(copy)

    mine = small_out.at[core, y, x]
    for d in (1, -1):
        small(small_ref, mine, near('x', d))
    for c in both:
        full(c, 0, 0)
    for c in both:
        full(c, 1, 0)
    for c in both:
        across(c, 0, 0)
    for c in both:
        wait_full(c, 0, 0)
        onward(c, 0, 0)
    for dp in (-1, 1):
        for c in both:
            full(c, 1, dp)
            across(c, dp, 0)
    smalls[0].wait_recv()
    smalls[1].wait_recv()
    left = small_out.at[core, y, at_x(-1)]
    small(left, left, near('x', 1))
    for b, fill in fills:
        if b > 0:
            fill.wait()
    for b in range(1, len(loads)):
        stores.append(pltpu.make_async_copy(bufs[b], packed[b - 1], store_sem.at[1 + b]))
        stores[-1].start()
    for c in both:
        wait_full(c, 1, 0)
        onward(c, 1, 0)
        across(c, 0, -1)
        across(c, 0, 1)
    for c in both:
        wait_part(c, 0, 0)
        full(c, 1, 2)
        across(c, 2, 0)
    for dp in (-1, 1):
        for c in both:
            wait_full(c, 1, dp)
            onward(c, 1, dp)
            across(c, dp, -1)
            across(c, dp, 1)
        if dp == -1:
            smalls[2].wait_recv()
            stores[1].wait()
            row = small_out.at[core, y]
            for d in (1, -1):
                small(row, row, near('y', d))
        else:
            smalls[3].wait_recv()
            smalls[4].wait_recv()
            below = small_out.at[core, at_y(-1)]
            small(below, below, near('y', 1))
    for c in both:
        wait_part(c, 1, 0)
        across(c, 0, 2)
    for c in both:
        wait_full(c, 1, 2)
        onward(c, 1, 2)
        across(c, 2, -1)
        across(c, 2, 1)
    smalls[5].wait_recv()
    small(small_out.at[core], small_out.at[core], partner)
    for dp in (-1, 1, 2):
        for c in both:
            wait_part(c, 1, dp)
            across(c, dp, 2)
    for key in order:
        if key[1] == 'core':
            sends[key].wait_recv()
    smalls[6].wait_recv()
    for key in order:
        sends[key].wait_send()
    for copy in smalls:
        copy.wait_send()
    for i, store in enumerate(stores):
        if i != 1:
            store.wait()


def gather_first(ny, nx, arrays, small, loads):
    rows = arrays[0].shape[-2]
    widths = [sum(p[3] for p in pieces) for pieces in loads]
    hbm = pl.BlockSpec(memory_space=pltpu.HBM)
    shapes = [jax.ShapeDtypeStruct((ny * nx * 2, rows, widths[0]), jnp.bfloat16), jax.ShapeDtypeStruct((2, ny, nx) + small.shape, small.dtype)]
    shapes += [jax.ShapeDtypeStruct((rows, w), jnp.bfloat16) for w in widths[1:]]
    copies = 2 * (4 + 16 + 16)
    return pl.pallas_call(
        functools.partial(gather_kernel, ny, nx, loads, len(arrays)),
        out_shape=shapes,
        in_specs=[hbm] * len(arrays) + [pl.BlockSpec(memory_space=pltpu.VMEM)],
        out_specs=[hbm] * len(shapes),
        scratch_shapes=[pltpu.VMEM((rows, w), jnp.bfloat16) for w in widths] + [
            pltpu.SemaphoreType.DMA((sum(len(p) for p in loads),)),
            pltpu.SemaphoreType.DMA((1 + len(loads),)),
            pltpu.SemaphoreType.DMA((copies,)),
            pltpu.SemaphoreType.DMA((copies,)),
            pltpu.SemaphoreType.DMA((7,)),
            pltpu.SemaphoreType.DMA((7,)),
        ],
        compiler_params=pltpu.CompilerParams(collective_id=0, has_side_effects=True, vmem_limit_bytes=32 * 1024 * 1024),
        cost_estimate=pl.CostEstimate(flops=2 * 10 ** 11, bytes_accessed=2 * ny * nx * 2 * rows * widths[0] * 2, transcendentals=0),
    )(*arrays, small)


def solution(mesh):
    rows_spec = P(('dp', 'fsdp'), None, None)
    in_specs = (rows_spec, P(('dp', 'fsdp')), P(None, 'fsdp', None, 'tp', None), P(None, None, ('tp', 'fsdp')), P(None, ('tp', 'fsdp'), None), P(None, 'fsdp', 'tp'), P(None, ('tp', 'fsdp')), P(None, ('tp', 'fsdp'), None), P(None, None, 'fsdp'), P(None, None, 'fsdp'))
    tp = mesh.shape['tp']
    fs = mesh.shape['fsdp']

    def per_device(hidden, seq_lens, w_qkv, b_qkv, w_proj, w_up, b_up, w_down, b_resid, ln_params):
        n_layers, rows, _, local_heads, head_dim = w_qkv.shape
        seq_len, d_model = hidden.shape[1:]
        share = local_heads * head_dim
        ff = w_up.shape[2]
        proj_rows = w_proj.shape[1]
        my_seqs = hidden.shape[0] // tp
        me = lax.axis_index('tp')

        def gather(x):
            return lax.all_gather(with_layout_constraint(x, Layout(major_to_minor=tuple(range(x.ndim)))), BOTH, axis=0, tiled=False)

        qkv_loc = [w_qkv[l].reshape(rows, 3 * share) for l in range(n_layers)]
        groups = rows // proj_rows
        proj_loc = [w_proj[l].reshape(proj_rows, groups, -1).transpose(1, 0, 2).reshape(rows, -1) for l in range(n_layers)]
        assert proj_loc[0].shape[1] == TILE and n_layers == 2
        wide_tiles = d_model // TILE
        ff_tiles = ff // TILE
        qkv_tiles = 3 * share // TILE
        f32 = jnp.float32
        small = jnp.concatenate([v.astype(f32).reshape(-1) for v in (ln_params, b_resid, b_qkv, b_up)])
        used = small.size
        small = jnp.pad(small, (0, -used % 1024)).reshape(-1, 128)
        loads = (
            ((0, 0, 0, ff, 0), (1, 0, 0, d_model, ff), (2, None, 0, 3 * share, ff + d_model), (4, None, 0, TILE, ff + d_model + 3 * share)),
            ((0, 1, 0, ff, 0), (3, None, 0, 3 * share, ff), (5, None, 0, TILE, ff + 3 * share)),
        )
        g1, small, local2 = gather_first(tp, fs // 2, (w_up, w_down, qkv_loc[0], qkv_loc[1], proj_loc[0], proj_loc[1]), small, loads)
        g2 = gather(local2)
        g3 = gather(lax.optimization_barrier((w_down[1], local2))[0])
        qkv_at = [(g1, ff_tiles + wide_tiles), (g2, ff_tiles)]
        proj_at = [(g1, ff_tiles + wide_tiles + qkv_tiles), (g2, ff_tiles + qkv_tiles)]
        down_at = [(g1, ff_tiles), (g3, 0)]

        small = small.reshape(2, tp, fs // 2, -1).transpose(1, 2, 0, 3).reshape(tp, fs, -1)
        piece = share // fs
        cuts = [0]
        for v in (ln_params, b_resid, b_qkv, b_up):
            cuts.append(cuts[-1] + v.size)
        ln_full = small[0, :, :cuts[1]].reshape((fs,) + ln_params.shape).transpose(1, 2, 0, 3).reshape(n_layers, ln_params.shape[1], -1)
        resid = small[0, :, cuts[1]:cuts[2]].reshape((fs,) + b_resid.shape).transpose(1, 2, 0, 3).reshape(n_layers, b_resid.shape[1], -1)
        wide = jnp.concatenate([ln_full, resid], axis=1)
        qkv_bias = small[..., cuts[2]:cuts[3]].reshape(tp, fs, n_layers, 3, piece).transpose(2, 0, 3, 1, 4).reshape(n_layers, -1)
        up_bias = small[..., cuts[3]:cuts[4]].reshape(tp, fs, n_layers, -1).transpose(2, 0, 1, 3).reshape(n_layers, -1)

        current = lax.dynamic_slice_in_dim(hidden, me * my_seqs, my_seqs, 0).reshape(my_seqs * seq_len, d_model)
        lens = lax.dynamic_slice_in_dim(seq_lens, me * my_seqs, my_seqs, 0)

        for l in range(n_layers):
            w, c0 = qkv_at[l]
            qkv = matmul(current, w, qkv_bias[l], tp * 3 * share, 1, (fs, rows, TILE), lambda j, k, c0=c0: (j // qkv_tiles, 0, c0 + j % qkv_tiles), norm=wide[l, :2])
            context = attend(qkv.reshape(my_seqs, seq_len, -1), lens, share, head_dim)
            w, c0 = proj_at[l]
            mid = matmul(context.reshape(my_seqs * seq_len, -1), w, wide[l, 4], d_model, 1, (tp * fs, proj_rows, TILE), lambda j, k, c0=c0: (0, j, c0), resid=current)
            u = matmul(mid, (g1, g2)[l], up_bias[l], tp * ff, 1, (fs, rows, TILE), lambda j, k: (j // ff_tiles, 0, j % ff_tiles), relu=True, norm=wide[l, 2:4])
            w, c0 = down_at[l]
            block = 2 * TILE if l == 0 else TILE
            steps, vmem = (2 * tp, 60) if l == 0 else (tp, 48)
            down = lambda first, n: matmul(u, w, wide[l, 5], n, steps, (tp * fs // steps, rows, block), lambda j, k: (k, 0, c0 * TILE // block + first + j), resid=mid, first=first, vmem=vmem)
            if l + 1 < n_layers:
                current = down(0, d_model)
        plus = [(i, (i + 1) % tp) for i in range(tp)]
        minus = [(i, (i - 1) % tp) for i in range(tp)]
        blocks = []
        for j in range(wide_tiles):
            own = down(j, TILE)
            right = lax.ppermute(own, 'tp', plus)
            left = lax.ppermute(own, 'tp', minus)
            blocks += [(0, j, own), (-1, j, right), (1, j, left)]
        for j in range(wide_tiles):
            here, perm = (blocks[3 * j + 1], plus) if j < wide_tiles // 2 else (blocks[3 * j + 2], minus)
            blocks.append((2, j, lax.ppermute(here[2], 'tp', perm)))
        near = 3 * wide_tiles
        out = None
        total = tp * my_seqs * seq_len
        pick = lambda *which: [blocks[i] for i in which]
        for group in (pick(*range(6)), pick(*range(6, near)), pick(near, near + 2), pick(near + 1, near + 3)):
            out = place(out, group, tp, total, d_model)
        return out.reshape(hidden.shape)

    return jax.shard_map(per_device, mesh=mesh, in_specs=in_specs, out_specs=rows_spec, check_vma=False)
```

```python
import functools

import jax
import jax.numpy as jnp
from jax import lax
from jax.experimental import pallas as pl
from jax.experimental.layout import Layout, with_layout_constraint
from jax.experimental.pallas import tpu as pltpu
from jax.sharding import PartitionSpec as P


BOTH = ('tp', 'fsdp')
TILE = 512


def layer_norm(acts_in, ln_gain, ln_shift):
    as_f32 = acts_in.astype(jnp.float32)
    row_mean = jnp.mean(as_f32, axis=-1, keepdims=True)
    centered = as_f32 - row_mean
    row_var = jnp.mean(centered * centered, axis=-1, keepdims=True)
    return (centered * lax.rsqrt(row_var + 1e-5) * ln_gain + ln_shift).astype(jnp.bfloat16)


def attn_kernel(head_dim, heads, lens_ref, q_ref, k_ref, v_ref, o_ref):
    seq_len = q_ref.shape[1]
    half = seq_len // 2
    length = lens_ref[pl.program_id(0)]
    last = jnp.minimum(lax.broadcasted_iota(jnp.int32, (1, seq_len), 1), length - 1)
    key = lax.broadcasted_iota(jnp.int32, (half, seq_len), 0)
    early_ok = key <= last
    late_ok = key[:, :half] + half <= last[:, half:]
    keys_by_queries = (((1,), (1,)), ((), ()))
    over_keys = (((0,), (0,)), ((), ()))
    columns = [slice(h * head_dim, (h + 1) * head_dim) for h in range(heads)]
    scores = []
    for c in columns:
        q = q_ref[0, :, c] * jnp.bfloat16(head_dim ** -0.5)
        early = lax.dot_general(k_ref[0, :half, c], q, keys_by_queries, preferred_element_type=jnp.float32)
        late = lax.dot_general(k_ref[0, half:, c], q[half:], keys_by_queries, preferred_element_type=jnp.float32)
        scores.append((early, late))
    outs = []
    for c, (early, late) in zip(columns, scores):
        early = jnp.where(early_ok, early, -1e30)
        late = jnp.where(late_ok, late, -1e30)
        top = jnp.max(early, axis=0, keepdims=True)
        late_top = jnp.maximum(top[:, half:], jnp.max(late, axis=0, keepdims=True))
        early = jnp.exp(early - jnp.concatenate([top[:, :half], late_top], axis=1))
        late = jnp.exp(late - late_top)
        total = jnp.sum(early, axis=0, keepdims=True)
        late_total = total[:, half:] + jnp.sum(late, axis=0, keepdims=True)
        scale = 1.0 / jnp.concatenate([total[:, :half], late_total], axis=1)
        early = (early * scale).astype(jnp.bfloat16)
        late = (late * scale[:, half:]).astype(jnp.bfloat16)
        v = v_ref[0, :, c]
        first = lax.dot_general(v[:half], early[:, :half], over_keys, preferred_element_type=jnp.float32)
        second = lax.dot_general(v, jnp.concatenate([early[:, half:], late], axis=0), over_keys, preferred_element_type=jnp.float32)
        outs.append(jnp.concatenate([first, second], axis=1))
    o_ref[0] = jnp.concatenate(outs, axis=0).T.astype(jnp.bfloat16)


def attend(qkv, lens, share, head_dim):
    seqs, seq_len, total = qkv.shape
    width = total // 3
    block = 256
    per = share // block
    spec = lambda part: pl.BlockSpec((1, seq_len, block), lambda s, g, h, lens: (s, 0, (g * 3 + part) * per + h))
    return pl.pallas_call(
        functools.partial(attn_kernel, head_dim, block // head_dim),
        out_shape=jax.ShapeDtypeStruct((seqs, seq_len, width), jnp.bfloat16),
        grid_spec=pltpu.PrefetchScalarGridSpec(
            num_scalar_prefetch=1,
            grid=(seqs, width // share, per),
            in_specs=[spec(0), spec(1), spec(2)],
            out_specs=pl.BlockSpec((1, seq_len, block), lambda s, g, h, lens: (s, 0, g * per + h)),
        ),
        compiler_params=pltpu.CompilerParams(vmem_limit_bytes=60 * 1024 * 1024),
        cost_estimate=pl.CostEstimate(flops=16 * seqs * seq_len * seq_len * width, bytes_accessed=8 * seqs * seq_len * width, transcendentals=seqs * seq_len * seq_len * width // head_dim),
    )(lens, qkv, qkv, qkv)


def mm_kernel(relu, steps, has_resid, has_norm, x_ref, w_ref, b_ref, *refs):
    resid_ref = refs[0] if has_resid else None
    o_ref, acc_ref = refs[-2:]
    k = pl.program_id(1)
    if has_norm:
        ln_ref, raw_ref, x_ref = refs[0], x_ref, acc_ref
        chunk = 128

        @pl.when(pl.program_id(0) == 0)
        def _():
            def normalise(i, carry):
                r = pl.ds(pl.multiple_of(i * chunk, chunk), chunk)
                x_ref[r, :] = layer_norm(raw_ref[r, :], ln_ref[0:1, :], ln_ref[1:2, :])
                return carry

            lax.fori_loop(0, raw_ref.shape[0] // chunk, normalise, 0)

    rows = x_ref.shape[0]
    w = w_ref[...].reshape(-1, w_ref.shape[2])
    half = min(512, rows)

    def start(r):
        base = jnp.broadcast_to(b_ref[...], (half, w.shape[1]))
        return base if resid_ref is None else base + resid_ref[r, :].astype(jnp.float32)

    for r0 in range(0, rows, half):
        r = pl.ds(r0, half)
        if steps == 1:
            total = jnp.dot(x_ref[r, :], w, preferred_element_type=jnp.float32) + start(r)
            o_ref[r, :] = (jnp.maximum(total, 0.0) if relu else total).astype(o_ref.dtype)
            continue

        @pl.when(k == 0)
        def _():
            acc_ref[r, :] = start(r)

        acc_ref[r, :] += jnp.dot(x_ref[r, :], w, preferred_element_type=jnp.float32)

        @pl.when(k == steps - 1)
        def _():
            o_ref[r, :] = acc_ref[r, :].astype(o_ref.dtype)


def matmul(x, w, bias, n, steps, w_block, w_index, resid=None, relu=False, first=0, tiles=None, norm=None, vmem=60):
    rows, depth = x.shape
    tile = w_block[2]
    in_specs = [
        pl.BlockSpec((rows, depth // steps), lambda j, k: (0, k)),
        pl.BlockSpec(w_block, w_index),
        pl.BlockSpec((1, tile), lambda j, k: (0, first + j)),
    ]
    args = [x, w, bias.reshape(1, -1)]
    if resid is not None:
        in_specs.append(pl.BlockSpec((rows, tile), lambda j, k: (0, first + j)))
        args.append(resid)
    scratch = pltpu.VMEM((rows, tile) if steps > 1 else (8, 128), jnp.float32)
    if norm is not None:
        in_specs.append(pl.BlockSpec((2, depth), lambda j, k: (0, 0)))
        args.append(norm)
        scratch = pltpu.VMEM((rows, depth), jnp.bfloat16)
    tiles = tiles or n // tile
    return pl.pallas_call(
        functools.partial(mm_kernel, relu, steps, resid is not None, norm is not None),
        out_shape=jax.ShapeDtypeStruct((rows, n), jnp.bfloat16),
        grid=(tiles, steps),
        in_specs=in_specs,
        out_specs=pl.BlockSpec((rows, tile), lambda j, k: (0, j)),
        scratch_shapes=[scratch],
        compiler_params=pltpu.CompilerParams(vmem_limit_bytes=vmem * 1024 * 1024),
        cost_estimate=pl.CostEstimate(flops=2 * rows * depth * tiles * tile, bytes_accessed=2 * (depth * tiles * tile + rows * (depth + tiles * tile)), transcendentals=0),
    )(*args)


def place(out, blocks, size, total, width):
    n = len(blocks)
    rows, tile = blocks[0][2].shape

    def kernel(*refs):
        o_ref, sems = refs[-2:]
        copies = []
        for i, (step, column, _) in enumerate(blocks):
            owner = lax.rem(lax.axis_index('tp') + step + size, size)
            row = pl.multiple_of(owner * rows, rows)
            copy = pltpu.make_async_copy(refs[i], o_ref.at[pl.ds(row, rows), pl.ds(column * tile, tile)], sems.at[i])
            copy.start()
            copies.append(copy)
        for copy in copies:
            copy.wait()

    whole = pl.BlockSpec(memory_space=pltpu.HBM)
    args = [x for _, _, x in blocks] + ([] if out is None else [out])
    return pl.pallas_call(
        kernel,
        out_shape=jax.ShapeDtypeStruct((total, width), args[0].dtype),
        in_specs=[pl.BlockSpec(memory_space=pltpu.VMEM)] * n + ([] if out is None else [whole]),
        out_specs=whole,
        scratch_shapes=[pltpu.SemaphoreType.DMA((n,))],
        input_output_aliases={} if out is None else {n: 0},
        compiler_params=pltpu.CompilerParams(vmem_limit_bytes=24 * 1024 * 1024),
        cost_estimate=pl.CostEstimate(flops=n * rows * tile, bytes_accessed=4 * n * rows * tile, transcendentals=0),
    )(*args)


def gather_kernel(ny, nx, loads, n_in, own, *refs):
    n_buf = len(loads) + own
    ins = refs[:n_in]
    small_ref = refs[n_in]
    out, small_out, *packed = refs[n_in + 1:n_in + 2 + n_buf]
    rest = refs[n_in + 2 + n_buf:]
    bufs, (load_sem, store_sem, send_sem, recv_sem, small_send, small_recv) = rest[:n_buf], rest[n_buf:]
    shard = bufs[0]
    rows = shard.shape[0]
    y = lax.axis_index('tp')
    f = lax.axis_index('fsdp')
    x = lax.div(f, 2)
    core = lax.rem(f, 2)
    at_y = lambda d: lax.rem(y + d + ny, ny)
    at_x = lambda d: lax.rem(x + d + nx, nx)
    slot = lambda dy, dx: (at_y(dy) * nx + at_x(dx)) * 2 + core
    near = lambda dim, d: {'tp': at_y(d), 'fsdp': f} if dim == 'y' else {'tp': y, 'fsdp': at_x(d) * 2 + core}
    partner = {'tp': y, 'fsdp': x * 2 + 1 - core}

    barrier = pltpu.get_barrier_semaphore()
    for dev in (near('x', 1), near('x', -1), near('y', 1), near('y', -1), partner):
        pl.semaphore_signal(barrier, inc=1, device_id=dev, device_id_type=pl.DeviceIdType.MESH)

    fills = []
    for b, pieces in enumerate(loads):
        for which, layer, c0, width, d0 in pieces:
            src = ins[which] if layer is None else ins[which].at[layer]
            fills.append((b, pltpu.make_async_copy(src.at[:, pl.ds(c0, width)], bufs[b].at[:, pl.ds(d0, width)], load_sem.at[len(fills)])))
    if own:
        mine = bufs[-1].shape[0]
        fills.append((n_buf - 1, pltpu.make_async_copy(ins[-1].at[pl.ds(pl.multiple_of(y * mine, mine), mine)], bufs[-1], load_sem.at[len(fills)])))
    for _, fill in fills:
        fill.start()
    for b, fill in fills:
        if b == 0:
            fill.wait()
    stores = [pltpu.make_async_copy(shard, out.at[slot(0, 0)], store_sem.at[0]),
              pltpu.make_async_copy(small_ref, small_out.at[core, y, x], store_sem.at[1])]
    for store in stores:
        store.start()
    pl.semaphore_wait(barrier, 5)

    sends = {}
    order = []

    def send(key, dev, dp, dq, r0, n):
        colour = key[0]
        where = slot(dq, dp) if colour == 0 else slot(dp, dq)
        r = pl.ds(colour * (rows // 2) + r0, n)
        src = shard.at[r] if (dp, dq) == (0, 0) else out.at[where, r]
        i = len(order)
        copy = pltpu.make_async_remote_copy(src, out.at[where, r], send_sem.at[i], recv_sem.at[i], device_id=dev, device_id_type=pl.DeviceIdType.MESH)
        copy.start()
        sends[key] = copy
        order.append(key)

    half, quarter = rows // 2, rows // 4
    dims = ('xy', 'yx')
    got = lambda *key: sends[key].wait_recv()

    def full(c, phase, dp):
        for d in (1, -1):
            send((c, phase, dp, d, 'full'), near(dims[c][phase], d), dp, 0, 0, half)

    def onward(c, phase, dp):
        for d, r0 in ((1, 0), (-1, quarter)):
            pos = (-d, 0) if phase == 0 else (dp, -d)
            send((c, phase, dp, d, 'part'), near(dims[c][phase], d), *pos, r0, quarter)

    def wait_full(c, phase, dp):
        got(c, phase, dp, 1, 'full')
        got(c, phase, dp, -1, 'full')

    def wait_part(c, phase, dp):
        got(c, phase, dp, 1, 'part')
        got(c, phase, dp, -1, 'part')

    def across(c, dp, dq):
        send((c, 'core', dp, dq), partner, dp, dq, 0, half)

    both = (0, 1)
    smalls = []

    def small(src, dst, dev):
        i = len(smalls)
        copy = pltpu.make_async_remote_copy(src, dst, small_send.at[i], small_recv.at[i], device_id=dev, device_id_type=pl.DeviceIdType.MESH)
        copy.start()
        smalls.append(copy)

    mine = small_out.at[core, y, x]
    for d in (1, -1):
        small(small_ref, mine, near('x', d))
    for c in both:
        full(c, 0, 0)
    for c in both:
        full(c, 1, 0)
    for c in both:
        across(c, 0, 0)
    for c in both:
        wait_full(c, 0, 0)
        onward(c, 0, 0)
    for dp in (-1, 1):
        for c in both:
            full(c, 1, dp)
            across(c, dp, 0)
    smalls[0].wait_recv()
    smalls[1].wait_recv()
    left = small_out.at[core, y, at_x(-1)]
    small(left, left, near('x', 1))
    for b, fill in fills:
        if b > 0:
            fill.wait()
    for b in range(1, n_buf):
        stores.append(pltpu.make_async_copy(bufs[b], packed[b - 1], store_sem.at[1 + b]))
        stores[-1].start()
    for c in both:
        wait_full(c, 1, 0)
        onward(c, 1, 0)
        across(c, 0, -1)
        across(c, 0, 1)
    for c in both:
        wait_part(c, 0, 0)
        full(c, 1, 2)
        across(c, 2, 0)
    for dp in (-1, 1):
        for c in both:
            wait_full(c, 1, dp)
            onward(c, 1, dp)
            across(c, dp, -1)
            across(c, dp, 1)
        if dp == -1:
            smalls[2].wait_recv()
            stores[1].wait()
            row = small_out.at[core, y]
            for d in (1, -1):
                small(row, row, near('y', d))
        else:
            smalls[3].wait_recv()
            smalls[4].wait_recv()
            below = small_out.at[core, at_y(-1)]
            small(below, below, near('y', 1))
    for c in both:
        wait_part(c, 1, 0)
        across(c, 0, 2)
    for c in both:
        wait_full(c, 1, 2)
        onward(c, 1, 2)
        across(c, 2, -1)
        across(c, 2, 1)
    smalls[5].wait_recv()
    small(small_out.at[core], small_out.at[core], partner)
    for dp in (-1, 1, 2):
        for c in both:
            wait_part(c, 1, dp)
            across(c, dp, 2)
    for key in order:
        if key[1] == 'core':
            sends[key].wait_recv()
    smalls[6].wait_recv()
    for key in order:
        sends[key].wait_send()
    for copy in smalls:
        copy.wait_send()
    for i, store in enumerate(stores):
        if i != 1:
            store.wait()


def gather_first(ny, nx, arrays, small, loads, own, collective_id):
    rows = arrays[0].shape[-2]
    widths = [sum(p[3] for p in pieces) for pieces in loads]
    hbm = pl.BlockSpec(memory_space=pltpu.HBM)
    local = [(rows, w) for w in widths]
    if own:
        local.append((arrays[-1].shape[0] // ny, arrays[-1].shape[1]))
    shapes = [jax.ShapeDtypeStruct((ny * nx * 2, rows, widths[0]), jnp.bfloat16), jax.ShapeDtypeStruct((2, ny, nx) + small.shape, small.dtype)]
    shapes += [jax.ShapeDtypeStruct(shape, jnp.bfloat16) for shape in local[1:]]
    copies = 2 * (4 + 16 + 16)
    sizes = (sum(len(p) for p in loads) + own, 1 + len(local), copies, copies, 7, 7)
    return pl.pallas_call(
        functools.partial(gather_kernel, ny, nx, loads, len(arrays), own),
        out_shape=shapes,
        in_specs=[hbm] * len(arrays) + [pl.BlockSpec(memory_space=pltpu.VMEM)],
        out_specs=[hbm] * len(shapes),
        scratch_shapes=[pltpu.VMEM(shape, jnp.bfloat16) for shape in local] + [pltpu.SemaphoreType.DMA((n,)) for n in sizes],
        compiler_params=pltpu.CompilerParams(collective_id=collective_id, has_side_effects=True, vmem_limit_bytes=60 * 1024 * 1024),
        cost_estimate=pl.CostEstimate(flops=32 * rows * widths[0] * ny * nx, bytes_accessed=8 * ny * nx * rows * widths[0], transcendentals=0),
    )(*arrays, small)


def solution(mesh):
    rows_spec = P(('dp', 'fsdp'), None, None)
    in_specs = (rows_spec, P(('dp', 'fsdp')), P(None, 'fsdp', None, 'tp', None), P(None, None, ('tp', 'fsdp')), P(None, ('tp', 'fsdp'), None), P(None, 'fsdp', 'tp'), P(None, ('tp', 'fsdp')), P(None, ('tp', 'fsdp'), None), P(None, None, 'fsdp'), P(None, None, 'fsdp'))
    tp = mesh.shape['tp']
    fs = mesh.shape['fsdp']

    def per_device(hidden, seq_lens, w_qkv, b_qkv, w_proj, w_up, b_up, w_down, b_resid, ln_params):
        n_layers, rows, _, local_heads, head_dim = w_qkv.shape
        seq_len, d_model = hidden.shape[1:]
        share = local_heads * head_dim
        ff = w_up.shape[2]
        proj_rows = w_proj.shape[1]
        my_seqs = hidden.shape[0] // tp
        me = lax.axis_index('tp')

        def gather(x):
            return lax.all_gather(with_layout_constraint(x, Layout(major_to_minor=tuple(range(x.ndim)))), BOTH, axis=0, tiled=False)

        qkv_loc = [w_qkv[l].reshape(rows, 3 * share) for l in range(n_layers)]
        groups = rows // proj_rows
        proj_loc = [w_proj[l].reshape(proj_rows, groups, -1).transpose(1, 0, 2).reshape(rows, -1) for l in range(n_layers)]
        assert proj_loc[0].shape[1] == TILE and n_layers == 2
        wide_tiles = d_model // TILE
        ff_tiles = ff // TILE
        qkv_tiles = 3 * share // TILE
        f32 = jnp.float32
        small = jnp.concatenate([v.astype(f32).reshape(-1) for v in (ln_params, b_resid, b_qkv, b_up)])
        used = small.size
        small = jnp.pad(small, (0, -used % 1024)).reshape(-1, 128)
        loads = (
            ((0, 0, 0, ff, 0), (1, 0, 0, d_model, ff), (2, None, 0, 3 * share, ff + d_model)),
            ((0, 1, 0, ff, 0), (3, None, 0, 3 * share, ff), (4, None, 0, TILE, ff + 3 * share)),
            ((1, 1, 0, d_model, 0),),
        )
        rows_all = hidden.reshape(-1, d_model)
        g1, token, local2, local3, current = gather_first(tp, fs // 2, (w_up, w_down, qkv_loc[0], qkv_loc[1], proj_loc[1], rows_all), jnp.zeros((8, 128), f32), loads, 1, 0)
        proj0, small, token, g1, local2, local3 = lax.optimization_barrier((proj_loc[0], small, token, g1, local2, local3))
        g2 = gather(local2)
        g3 = gather(lax.optimization_barrier((local3, local2))[0])
        g0, small = gather_first(tp, fs // 2, (proj0,), small, (((0, None, 0, TILE, 0),),), 0, 1)
        qkv_at = [(g1, ff_tiles + wide_tiles), (g2, ff_tiles)]
        proj_at = [(g0, 0), (g2, ff_tiles + qkv_tiles)]
        down_at = [(g1, ff_tiles), (g3, 0)]

        small = small.reshape(2, tp, fs // 2, -1).transpose(1, 2, 0, 3).reshape(tp, fs, -1)
        piece = share // fs
        cuts = [0]
        for v in (ln_params, b_resid, b_qkv, b_up):
            cuts.append(cuts[-1] + v.size)
        ln_full = small[0, :, :cuts[1]].reshape((fs,) + ln_params.shape).transpose(1, 2, 0, 3).reshape(n_layers, ln_params.shape[1], -1)
        resid = small[0, :, cuts[1]:cuts[2]].reshape((fs,) + b_resid.shape).transpose(1, 2, 0, 3).reshape(n_layers, b_resid.shape[1], -1)
        wide = jnp.concatenate([ln_full, resid], axis=1)
        qkv_bias = small[..., cuts[2]:cuts[3]].reshape(tp, fs, n_layers, 3, piece).transpose(2, 0, 3, 1, 4).reshape(n_layers, -1)
        up_bias = small[..., cuts[3]:cuts[4]].reshape(tp, fs, n_layers, -1).transpose(2, 0, 1, 3).reshape(n_layers, -1)

        lens = lax.dynamic_slice_in_dim(seq_lens, me * my_seqs, my_seqs, 0)

        for l in range(n_layers):
            w, c0 = qkv_at[l]
            qkv = matmul(current, w, qkv_bias[l], tp * 3 * share, 1, (fs, rows, TILE), lambda j, k, c0=c0: (j // qkv_tiles, 0, c0 + j % qkv_tiles), norm=wide[l, :2])
            context = attend(qkv.reshape(my_seqs, seq_len, -1), lens, share, head_dim)
            w, c0 = proj_at[l]
            mid = matmul(context.reshape(my_seqs * seq_len, -1), w, wide[l, 4], d_model, 1, (tp * fs, proj_rows, TILE), lambda j, k, c0=c0: (0, j, c0), resid=current)
            u = matmul(mid, (g1, g2)[l], up_bias[l], tp * ff, 1, (fs, rows, TILE), lambda j, k: (j // ff_tiles, 0, j % ff_tiles), relu=True, norm=wide[l, 2:4])
            w, c0 = down_at[l]
            block = 2 * TILE if l == 0 else TILE
            steps, vmem = (2 * tp, 60) if l == 0 else (tp, 48)
            down = lambda first, n: matmul(u, w, wide[l, 5], n, steps, (tp * fs // steps, rows, block), lambda j, k: (k, 0, c0 * TILE // block + first + j), resid=mid, first=first, vmem=vmem)
            if l + 1 < n_layers:
                current = down(0, d_model)
        plus = [(i, (i + 1) % tp) for i in range(tp)]
        minus = [(i, (i - 1) % tp) for i in range(tp)]
        blocks = []
        for j in range(wide_tiles):
            own = down(j, TILE)
            right = lax.ppermute(own, 'tp', plus)
            left = lax.ppermute(own, 'tp', minus)
            blocks += [(0, j, own), (-1, j, right), (1, j, left)]
        for j in range(wide_tiles):
            here, perm = (blocks[3 * j + 1], plus) if j < wide_tiles // 2 else (blocks[3 * j + 2], minus)
            blocks.append((2, j, lax.ppermute(here[2], 'tp', perm)))
        near = 3 * wide_tiles
        out = None
        total = tp * my_seqs * seq_len
        pick = lambda *which: [blocks[i] for i in which]
        for group in (pick(*range(6)), pick(*range(6, near)), pick(near, near + 2), pick(near + 1, near + 3)):
            out = place(out, group, tp, total, d_model)
        return out.reshape(hidden.shape)

    return jax.shard_map(per_device, mesh=mesh, in_specs=in_specs, out_specs=rows_spec, check_vma=False)
```
